32 devices in a mesh: rep: 2 (over y), gx: 16 (over z, x, core).
Axes of the slice: x: 2, y: 2, z: 4, core: 2. Of those that a mesh axis runs over, the one named last changes fastest.
Arguments:
- positions: float32 [3, 49152], P(None, ('rep', 'gx')), parts along dimension 1, may hold values from 0 to 96
- velocities: float32 [3, 49152], P(None, ('rep', 'gx')), parts along dimension 1, may hold values from -9 to 9
- atom_params: float32 [4, 49152], P(None, ('rep', 'gx')), parts along dimension 1, may hold values from -1 to 2, as said below
- pair_list: int32 [3, 540672], P(None, ('rep', 'gx')), parts along dimension 1, may hold values from 0 to 479, as said below
- pair_count: int32 [32], P(('rep', 'gx')), parts along dimension 0, may hold values from 2112 to 16896, as said below
- exclusion: int32 [4, 540672], P(None, ('rep', 'gx')), parts along dimension 1, may hold values from 0 to 65535, as said below
- halo_far: int32 [3072], P(('rep', 'gx')), parts along dimension 0, may hold values from 0 to 191, as said below
- box_lengths: float32 [6], P('rep'), parts along dimension 0, may hold values from 12 to 96
- extended_variables: float32 [8], P('rep'), parts along dimension 0, may hold values from -0.3 to 0.3
Outputs:
- forces: float32 [3, 49152], P(None, ('rep', 'gx')), parts along dimension 1
- new_velocities: float32 [3, 49152], P(None, ('rep', 'gx')), parts along dimension 1
- new_positions: float32 [3, 49152], P(None, ('rep', 'gx')), parts along dimension 1
- new_coupling: float32 [8], P('rep'), parts along dimension 0
The draws below stay inside these ranges and needn't reach their ends.
There are 2 independent parts, one for each index of `rep`. The reference program is written for one: setup_inputs(seed, part) draws one part's arguments, and reference() takes and returns one part's arrays. A program takes and returns all parts, laid end to end along the dimension named above; each array names one. Nothing has to cross between parts.
Inputs may be any that keep to these rules, and one draw needn't show every extreme that they name: `pair_list`: row 0 is a local cluster 0 to 191, row 1 a slot 0 to 479 of the slot table, row 2 an image code 0 to 8. Over each domain's used columns row 0 never falls (the list is grouped by its first cluster). Unused columns hold valid entries too. `pair_count`: at most 16896; some domain uses all 16896 columns in every draw. `exclusion`: each word holds 16 bits; bit 1 means the atom pair interacts. `halo_far`: 96 distinct local clusters of each domain. `atom_params`: rows 1 to 3 are positive.
All inputs are finite; a program needn't handle non-finite values.
Results may differ from the reference program's by a relative error of at most 0.0003.
Values sent between devices are 32-bit elements; how exact they have to be, the bound alone decides.
No kernel may reach another device: no remote copies, remote signals or barrier semaphores. Data moves between devices by JAX's collectives and lax.ppermute only.
A program may use at most 64 MiB of HBM per device.

```python
import math
import jax
import jax.numpy as jnp
import numpy as np
from jax import lax

LX = 2
LY = 12
LZ = 8
CAND = 88
ATOMS_DEV = 1536
PAIRS_DEV = 16896
COPY_PARTICLES = 24576
PAIRS = 270336
N_GX = 16


def candidate_offsets():
    result = [(0, 0, 0)]
    for shift_y in range(-2, 3):
        for shift_z in range(-2, 3):
            if shift_y > 0 or (shift_y == 0 and shift_z > 0):
                result.append((0, shift_y, shift_z))
    for shift_x in range(1, 4):
        for shift_y in range(-2, 3):
            for shift_z in range(-2, 3):
                result.append((shift_x, shift_y, shift_z))
    return np.array(result, np.int32)


def upper_words():
    result = []
    for word_place in range(4):
        packed_bits = 0
        for bit_place in range(16):
            number = word_place * 16 + bit_place
            if number % 8 > number // 8:
                packed_bits += 1 << bit_place
        result.append(packed_bits)
    return np.array(result, np.int32)


def cluster_sites(key):
    subkeys = jax.random.split(jax.random.fold_in(key, 101), N_GX)
    return jax.vmap(lambda single: jax.random.permutation(single, LX * LY * LZ))(subkeys).astype(jnp.int32)


def box_stretch(key):
    return jax.random.uniform(jax.random.fold_in(key, 202), (3,), jnp.float32, -0.02, 0.02)


def pair_counts(key):
    base_counts = jax.random.randint(jax.random.fold_in(key, 303), (N_GX,), PAIRS_DEV // 8, PAIRS_DEV // 2 + 1)
    dense_counts = jax.random.randint(jax.random.fold_in(key, 304), (N_GX,), 3 * PAIRS_DEV // 4, PAIRS_DEV + 1)
    dense_start = jax.random.randint(jax.random.fold_in(key, 305), (), 0, N_GX)
    distance = (jnp.arange(N_GX, dtype=jnp.int32) - dense_start) % N_GX
    counts = jnp.where(distance < max(N_GX // 8, 1), dense_counts, base_counts)
    return jnp.where(distance == 0, PAIRS_DEV, counts).astype(jnp.int32)


def pair_order(key):
    counts = pair_counts(key)
    subkeys = jax.random.split(jax.random.fold_in(key, 306), N_GX)
    ranks = jax.vmap(lambda single: jax.random.permutation(single, PAIRS_DEV))(subkeys)
    candidate = jnp.arange(PAIRS_DEV, dtype=jnp.int32)[None, :]
    sort_key = jnp.where(ranks < counts[:, None], candidate, candidate + PAIRS_DEV)
    return jnp.argsort(sort_key, axis=1).astype(jnp.int32)


def pair_tables(key):
    site_of = cluster_sites(key)
    cluster_at = jnp.argsort(site_of, axis=1).astype(jnp.int32)
    plane_size = LY * LZ
    clusters = LX * plane_size
    offsets = jnp.asarray(candidate_offsets())
    layer_x = (site_of // plane_size)[:, :, None]
    layer_y = (site_of // LZ % LY)[:, :, None]
    layer_z = (site_of % LZ)[:, :, None]
    target_x = layer_x + offsets[:, 0]
    raw_y = layer_y + offsets[:, 1]
    raw_z = layer_z + offsets[:, 2]
    wrap_y = (raw_y >= LY).astype(jnp.int32) - (raw_y < 0).astype(jnp.int32)
    wrap_z = (raw_z >= LZ).astype(jnp.int32) - (raw_z < 0).astype(jnp.int32)
    target_y = raw_y - wrap_y * LY
    target_z = raw_z - wrap_z * LZ
    image_code = (wrap_y + 1) * 3 + wrap_z + 1
    in_plane = target_y * LZ + target_z
    own_site = jnp.clip(target_x, 0, LX - 1) * plane_size + in_plane
    near_site = jnp.clip(target_x - LX, 0, LX - 1) * plane_size + in_plane
    next_at = jnp.roll(cluster_at, -1, axis=0)
    own_slot = jnp.take_along_axis(cluster_at, own_site.reshape(N_GX, -1), axis=1).reshape(own_site.shape)
    near_slot = clusters + jnp.take_along_axis(next_at, near_site.reshape(N_GX, -1), axis=1).reshape(near_site.shape)
    far_slot = 2 * clusters + in_plane
    second = jnp.where(target_x < LX, own_slot, jnp.where(target_x < 2 * LX, near_slot, far_slot))
    first = jnp.broadcast_to(jnp.arange(clusters, dtype=jnp.int32)[None, :, None], second.shape)
    is_self = jnp.broadcast_to((jnp.arange(CAND) == 0)[None, None, :], second.shape)
    tables = jnp.stack([first, second, image_code]).reshape(3, N_GX, clusters * CAND).astype(jnp.int32)
    return (tables, is_self.reshape(N_GX, clusters * CAND))


def draw_positions(key, part):
    site_of = cluster_sites(key)
    stretch = box_stretch(key)
    plane_size = LY * LZ
    layer_x = (site_of // plane_size)[:, :, None]
    layer_y = (site_of // LZ % LY)[:, :, None]
    layer_z = (site_of % LZ)[:, :, None]
    atom_slot = jnp.arange(8, dtype=jnp.int32)
    domain = jnp.arange(N_GX, dtype=jnp.int32)[:, None, None]
    coord_x = (domain * LX + layer_x) * 2 + atom_slot // 4
    coord_y = layer_y * 2 + atom_slot // 2 % 2
    coord_z = layer_z * 2 + atom_slot % 2
    lattice = jnp.stack([coord_x, coord_y, coord_z]).astype(jnp.float32).reshape(3, COPY_PARTICLES) + 0.5
    jitter = jax.random.uniform(jax.random.fold_in(key, 203), (3, COPY_PARTICLES), jnp.float32, -0.05, 0.05)
    return lattice * (1.0 + stretch[:, None]) + jitter


def draw_box_lengths(key, part):
    nominal = jnp.array([2.0 * LX * N_GX, 2.0 * LY, 2.0 * LZ], jnp.float32)
    return nominal * (1.0 + box_stretch(key))


def draw_velocities(key, part):
    domain = (jnp.arange(COPY_PARTICLES, dtype=jnp.int32) // ATOMS_DEV).astype(jnp.float32)
    spread = jnp.sqrt(1.0 + 2.0 * domain / (N_GX - 1))
    base = jnp.clip(jax.random.normal(jax.random.fold_in(key, 501), (3, COPY_PARTICLES), jnp.float32), -5.0, 5.0)
    return base * spread[None, :]


def draw_atom_params(key, part):
    charge = jax.random.uniform(jax.random.fold_in(key, 601), (COPY_PARTICLES,), jnp.float32, -1.0, 1.0)
    dispersion = jnp.exp(jax.random.uniform(jax.random.fold_in(key, 602), (COPY_PARTICLES,), jnp.float32, math.log(0.3), 0.0))
    repulsion = jnp.exp(jax.random.uniform(jax.random.fold_in(key, 603), (COPY_PARTICLES,), jnp.float32, math.log(0.1), math.log(0.3)))
    inverse_mass = jnp.exp(jax.random.uniform(jax.random.fold_in(key, 604), (COPY_PARTICLES,), jnp.float32, math.log(0.5), math.log(2.0)))
    return jnp.stack([charge, dispersion, repulsion, inverse_mass])


def draw_pair_list(key, part):
    tables, is_self = pair_tables(key)
    order = pair_order(key)
    return jnp.take_along_axis(tables, order[None, :, :], axis=2).reshape(3, PAIRS)


def draw_pair_count(key, part):
    return pair_counts(key)


def draw_exclusion(key, part):
    tables, is_self = pair_tables(key)
    order = pair_order(key)
    first_words = jax.random.randint(jax.random.fold_in(key, 401), (4, N_GX, PAIRS_DEV), 0, 65536)
    second_words = jax.random.randint(jax.random.fold_in(key, 402), (4, N_GX, PAIRS_DEV), 0, 65536)
    words = first_words | second_words
    upper = jnp.asarray(upper_words())[:, None, None]
    words = jnp.where(is_self[None, :, :], words & upper, words)
    return jnp.take_along_axis(words, order[None, :, :], axis=2).reshape(4, PAIRS).astype(jnp.int32)


def draw_halo_far(key, part):
    site_of = cluster_sites(key)
    cluster_at = jnp.argsort(site_of, axis=1).astype(jnp.int32)
    return cluster_at[:, :LY * LZ].reshape(N_GX * LY * LZ)


def setup_inputs(seed: int = 0, part: int = 0) -> dict:
    seeds = jax.random.split(jax.random.key(seed), 10)
    part_keys = jax.random.split(jax.random.fold_in(seeds[9], part), 10)
    return {
        "positions": draw_positions(jax.random.fold_in(jax.random.fold_in(seeds[9], part), 71), part),
        "velocities": draw_velocities(jax.random.fold_in(jax.random.fold_in(seeds[9], part), 71), part),
        "atom_params": draw_atom_params(jax.random.fold_in(jax.random.fold_in(seeds[9], part), 71), part),
        "pair_list": draw_pair_list(jax.random.fold_in(jax.random.fold_in(seeds[9], part), 71), part),
        "pair_count": draw_pair_count(jax.random.fold_in(jax.random.fold_in(seeds[9], part), 71), part),
        "exclusion": draw_exclusion(jax.random.fold_in(jax.random.fold_in(seeds[9], part), 71), part),
        "halo_far": draw_halo_far(jax.random.fold_in(jax.random.fold_in(seeds[9], part), 71), part),
        "box_lengths": draw_box_lengths(jax.random.fold_in(jax.random.fold_in(seeds[9], part), 71), part),
        "extended_variables": jnp.clip(jax.random.uniform(part_keys[8], (4,), jnp.float32, -0.3, 0.3), -0.3, 0.3),
    }


time_step = 0.25
reaction_term = 1.0 / 1331.0
thermal_scale_unit = 2.0
reservoir_inertia_mass = 4.0
barostat_gain = 0.1
pressure_target = 1.0

def pair_tiles(slot_table, pair_rows, word_rows, usable, box_lengths):
    tile_width = pair_rows.shape[1]
    first_rows = jnp.take(slot_table, pair_rows[0], axis=0).T.reshape(6, 8, tile_width)
    second_rows = jnp.take(slot_table, pair_rows[1], axis=0).T.reshape(6, 8, tile_width)
    image_y = (pair_rows[2] // 3 - 1).astype(jnp.float32) * box_lengths[1]
    image_z = (pair_rows[2] % 3 - 1).astype(jnp.float32) * box_lengths[2]
    delta_x = second_rows[0][None, :, :] - first_rows[0][:, None, :]
    delta_y = second_rows[1][None, :, :] - first_rows[1][:, None, :] + image_y
    delta_z = second_rows[2][None, :, :] - first_rows[2][:, None, :] + image_z
    shifts = (jnp.arange(64, dtype=jnp.int32) % 16)[:, None]
    mask_bits = jnp.right_shift(jnp.repeat(word_rows, 16, axis=0), shifts) & 1
    interact = (mask_bits.reshape(8, 8, tile_width) == 1) & usable[None, None, :]
    radius_sq = delta_x * delta_x + delta_y * delta_y + delta_z * delta_z
    radius_sq = jnp.where(interact, radius_sq, 1.0)
    inverse = lax.rsqrt(radius_sq)
    inverse_sq = inverse * inverse
    inverse_six = inverse_sq * inverse_sq * inverse_sq
    charge_pair = first_rows[3][:, None, :] * second_rows[3][None, :, :]
    dispersion = first_rows[4][:, None, :] * second_rows[4][None, :, :]
    repulsion = first_rows[5][:, None, :] * second_rows[5][None, :, :]
    scalar = charge_pair * (inverse * inverse_sq - reaction_term) + (12.0 * repulsion * inverse_six - 6.0 * dispersion) * inverse_six * inverse_sq
    scalar = jnp.where(interact, scalar, 0.0)
    components = (delta_x, delta_y, delta_z)
    onto_second = jnp.stack([lax.optimization_barrier(jnp.sum(scalar * component, axis=0)) for component in components])
    onto_first = -jnp.stack([lax.optimization_barrier(jnp.sum(scalar * component, axis=1)) for component in components])
    virial = -0.5 * jnp.stack([jnp.sum(scalar * component * component) for component in components])
    tile_terms = jnp.concatenate([onto_first.reshape(24, tile_width), onto_second.reshape(24, tile_width)], axis=1).T
    owners = jnp.concatenate([pair_rows[0], pair_rows[1]])
    return (tile_terms, owners, virial)

def device_forces(slot_table, pair_rows, word_rows, pair_total, box_lengths):
    slots = slot_table.shape[0]
    block_rows = PAIRS_DEV // LY
    starts = jnp.arange(LY, dtype=jnp.int32) * block_rows

    def one_block(running, first_row):
        accumulated, virial = running
        pair_block = lax.dynamic_slice_in_dim(pair_rows, first_row, block_rows, 1)
        word_block = lax.dynamic_slice_in_dim(word_rows, first_row, block_rows, 1)
        usable = first_row + jnp.arange(block_rows, dtype=jnp.int32) < pair_total
        tile_terms, owners, partial_value = pair_tiles(slot_table, pair_block, word_block, usable, box_lengths)
        accumulated = accumulated + jax.ops.segment_sum(tile_terms, owners, num_segments=slots)
        return ((accumulated, virial + partial_value), None)
    start_state = (jnp.zeros((slots, 24), jnp.float32), jnp.zeros((3,), jnp.float32))
    result, unused = lax.scan(one_block, start_state, starts)
    return result

def reference(positions, velocities, atom_params, pair_list, pair_count, exclusion, halo_far, box_lengths, extended_variables):
    clusters = LX * LY * LZ
    far_clusters = LY * LZ
    slots = 2 * clusters + far_clusters
    packed = jnp.concatenate([positions, atom_params[:3]], axis=0)
    packed = packed.reshape(6, N_GX, clusters, 8).transpose(1, 0, 2, 3)
    far_lists = halo_far.reshape(N_GX, far_clusters)
    far_rows = jax.vmap(lambda block_data, chosen: block_data[:, chosen, :])(packed, far_lists)
    domain = jnp.arange(N_GX, dtype=jnp.int32)
    near_rows = jnp.roll(packed, -1, axis=0)
    far_in = jnp.roll(far_rows, -2, axis=0)
    near_lift = jnp.where(domain == N_GX - 1, box_lengths[0], 0.0)
    far_lift = jnp.where(domain >= N_GX - 2, box_lengths[0], 0.0)
    near_rows = near_rows.at[:, 0].add(near_lift[:, None, None])
    far_in = far_in.at[:, 0].add(far_lift[:, None, None])
    tables = jnp.concatenate([packed, near_rows, far_in], axis=2)
    tables = tables.transpose(0, 2, 1, 3).reshape(N_GX, slots, 48)
    pair_blocks = pair_list.reshape(3, N_GX, PAIRS_DEV).transpose(1, 0, 2)
    word_blocks = exclusion.reshape(4, N_GX, PAIRS_DEV).transpose(1, 0, 2)

    def per_domain(item):
        return device_forces(item[0], item[1], item[2], item[3], box_lengths)
    accumulated, virials = lax.map(per_domain, (tables, pair_blocks, word_blocks, pair_count))
    own_part = accumulated[:, :clusters]
    near_back = jnp.roll(accumulated[:, clusters:2 * clusters], 1, axis=0)
    far_back = jnp.roll(accumulated[:, 2 * clusters:], 2, axis=0)
    summed = own_part + near_back
    summed = jax.vmap(lambda block_data, chosen, extra: block_data.at[chosen].add(extra))(summed, far_lists, far_back)
    forces = summed.reshape(N_GX, clusters, 3, 8).transpose(2, 0, 1, 3).reshape(3, COPY_PARTICLES)
    inverse_mass = atom_params[3]
    kinetic = 0.5 * lax.optimization_barrier(jnp.sum(velocities * velocities / inverse_mass[None, :], axis=1))
    virial = lax.optimization_barrier(jnp.sum(virials, axis=0))
    overall_motion_work = jnp.sum(kinetic)
    volume = box_lengths[0] * box_lengths[1] * box_lengths[2]
    thermal_ratio_value = 2.0 * overall_motion_work / (3.0 * COPY_PARTICLES * thermal_scale_unit)
    reservoir_damping = extended_variables[0] + reservoir_inertia_mass * (thermal_ratio_value - 1.0)
    box_rates = extended_variables[1:] + barostat_gain * (kinetic - virial - pressure_target * volume / 2.0) / (overall_motion_work / 3.0)
    new_velocities = velocities + time_step * (forces * inverse_mass[None, :] - (reservoir_damping + box_rates[:, None]) * velocities)
    new_positions = positions * (1.0 + time_step * box_rates[:, None]) + time_step * new_velocities
    new_coupling = jnp.concatenate([reservoir_damping[None], box_rates])
    return (forces, new_velocities, new_positions, new_coupling)
```

```python
import functools

import jax
import jax.numpy as jnp
from jax import lax
from jax.experimental import pallas as pl
from jax.experimental.pallas import tpu as pltpu
from jax.sharding import PartitionSpec as P

time_step = 0.25
reaction_term = 1.0 / 1331.0
thermal_scale_unit = 2.0
reservoir_inertia_mass = 4.0
barostat_gain = 0.1
pressure_target = 1.0

F32 = jnp.float32
BF16 = jnp.bfloat16
LANES = 128


def passed_along(value, axis, steps):
    count = lax.axis_size(axis)
    pairs = [(source, (source + steps) % count) for source in range(count)]
    return lax.ppermute(value, axis, pairs)


def split_bf16(value, terms):
    parts = []
    for _ in range(terms - 1):
        part = value.astype(BF16)
        parts.append(part)
        value = value - part.astype(F32)
    parts.append(value.astype(BF16))
    return parts


def one_hot_rows(index_row, rows):
    width = index_row.shape[1]
    numbers = lax.broadcasted_iota(jnp.int16, (rows, width), 0)
    wanted = jnp.broadcast_to(index_row, (rows, width)).astype(jnp.int16)
    return jnp.where(numbers == wanted, jnp.ones((), BF16), jnp.zeros((), BF16))


def fold_rows(first, second, stride, lane_rows):
    keep = (lane_rows & stride) == 0
    return jnp.where(keep, first, second) + pltpu.roll(
        jnp.where(keep, second, first), 8 - stride, 0
    )


def pair_kernel(
    count_ref, box_ref, table_ref, pair_ref, word_ref, force_ref, virial_ref, parts_ref, onto_j, onto_i, *, width
):
    slots = table_ref.shape[1]
    clusters = onto_i.shape[1]
    table = table_ref[...]
    places = split_bf16(table[:24], 3)
    params = split_bf16(table[24:], 2)
    parts_ref[...] = jnp.concatenate([part.astype(F32) for part in places + params], axis=0).astype(BF16)
    onto_j[...] = jnp.zeros_like(onto_j)
    onto_i[...] = jnp.zeros_like(onto_i)
    total = count_ref[0]
    box_y = box_ref[1]
    box_z = box_ref[2]
    lane_rows = lax.broadcasted_iota(jnp.int32, (8, LANES), 0)

    def gathered(hot, rows):
        raw = jnp.dot(parts_ref[:, :rows], hot, preferred_element_type=F32)
        place = raw[0:24] + (raw[24:48] + raw[48:72])
        param = raw[72:96] + raw[96:120]
        return place, param

    def one_block(block, virial):
        start = pl.multiple_of(block * width, width)
        first = pair_ref[0:1, pl.ds(start, width)]
        second = pair_ref[1:2, pl.ds(start, width)]
        image = pair_ref[2:3, pl.ds(start, width)]
        words = word_ref[:, pl.ds(start, width)]
        column = start + lax.broadcasted_iota(jnp.int32, (1, width), 1)
        words = jnp.where(column < total, words, 0)
        image_row = (image >= 3).astype(jnp.int32) + (image >= 6).astype(jnp.int32)
        shift_y = (image_row - 1).astype(F32) * box_y
        shift_z = (image - 3 * image_row - 1).astype(F32) * box_z
        hot_i = one_hot_rows(first, clusters)
        hot_j = one_hot_rows(second, slots)
        place_i, param_i = gathered(hot_i, clusters)
        place_j, param_j = gathered(hot_j, slots)
        j_chunks = []
        i_chunks = []
        for chunk in range(width // LANES):
            cut = slice(chunk * LANES, (chunk + 1) * LANES)
            jx = place_j[0:8, cut]
            jy = place_j[8:16, cut] + shift_y[:, cut]
            jz = place_j[16:24, cut] + shift_z[:, cut]
            jq = param_j[0:8, cut]
            je = 6.0 * param_j[8:16, cut]
            jb = 12.0 * param_j[16:24, cut]
            force_j = [jnp.zeros((8, LANES), F32) for _ in range(3)]
            stack = []
            for a in range(8):
                if a % 2 == 0:
                    shifted = jnp.right_shift(
                        jnp.broadcast_to(words[a // 2 : a // 2 + 1, cut], (8, LANES)), lane_rows
                    )
                interact = (shifted & (1 if a % 2 == 0 else 256)) != 0
                delta = (
                    jx - place_i[a : a + 1, cut],
                    jy - place_i[8 + a : 9 + a, cut],
                    jz - place_i[16 + a : 17 + a, cut],
                )
                radius_sq = delta[0] * delta[0] + delta[1] * delta[1] + delta[2] * delta[2]
                inverse = lax.rsqrt(radius_sq)
                inverse_sq = inverse * inverse
                inverse_six = inverse_sq * inverse_sq * inverse_sq
                charge = jq * param_i[a : a + 1, cut]
                dispersion = je * param_i[8 + a : 9 + a, cut]
                repulsion = jb * param_i[16 + a : 17 + a, cut]
                scalar = charge * (inverse * inverse_sq - reaction_term) + (
                    repulsion * inverse_six - dispersion
                ) * (inverse_six * inverse_sq)
                scalar = jnp.where(interact, scalar, 0.0)
                force = [scalar * part for part in delta]
                force_j = [old + new for old, new in zip(force_j, force)]
                virial = tuple(old + f * d for old, f, d in zip(virial, force, delta))
                stack.append((1, force))
                while len(stack) > 1 and stack[-1][0] == stack[-2][0]:
                    stride, high = stack.pop()
                    _, low = stack.pop()
                    stack.append(
                        (2 * stride, [fold_rows(x, y, stride, lane_rows) for x, y in zip(low, high)])
                    )
            j_chunks.append(jnp.concatenate(force_j, axis=0))
            i_chunks.append(jnp.concatenate(stack[0][1], axis=0))
        sides = ((j_chunks, hot_j, onto_j), (i_chunks, hot_i, onto_i))
        for chunks, hot, target in sides:
            high, low = split_bf16(jnp.concatenate(chunks, axis=1), 2)
            pieces = jnp.concatenate([high.astype(F32), low.astype(F32)], axis=0).astype(BF16)
            target[...] += lax.dot_general(
                pieces, hot, (((1,), (1,)), ((), ())), preferred_element_type=F32
            )
        return virial

    blocks = (total + width - 1) // width
    zero = jnp.zeros((8, LANES), F32)
    virial = lax.fori_loop(0, blocks, one_block, (zero, zero, zero))
    force_ref[...] = onto_j[0:24, :] + onto_j[24:48, :]
    force_ref[:, :clusters] = force_ref[:, :clusters] - (onto_i[0:24, :] + onto_i[24:48, :])
    virial_ref[...] = jnp.concatenate([-0.5 * part for part in virial], axis=0)


def pair_forces(pair_count, box_lengths, table, pair_list, exclusion, clusters):
    columns = pair_list.shape[1]
    width = next(w for w in (512, 256, 128) if columns % w == 0)
    slots = table.shape[1]
    vmem = pl.BlockSpec(memory_space=pltpu.VMEM)
    smem = pl.BlockSpec(memory_space=pltpu.SMEM)
    return pl.pallas_call(
        functools.partial(pair_kernel, width=width),
        out_shape=(
            jax.ShapeDtypeStruct((24, slots), F32),
            jax.ShapeDtypeStruct((24, LANES), F32),
        ),
        in_specs=[smem, smem, vmem, vmem, vmem],
        out_specs=(vmem, vmem),
        scratch_shapes=[
            pltpu.VMEM((120, slots), BF16),
            pltpu.VMEM((48, slots), F32),
            pltpu.VMEM((48, clusters), F32),
        ],
        name="pair_forces",
    )(pair_count, box_lengths, table, pair_list, exclusion)


def on_device(
    positions,
    velocities,
    atom_params,
    pair_list,
    pair_count,
    exclusion,
    halo_far,
    box_lengths,
    extended_variables,
):
    atoms_here = positions.shape[1]
    clusters = atoms_here // 8
    domain_index = lax.axis_index("gx")
    axis_count = lax.axis_size("gx")
    inverse_mass = atom_params[3]
    packed = jnp.concatenate([positions, atom_params[:3]], axis=0)
    own = packed.reshape(6, clusters, 8).transpose(0, 2, 1).reshape(48, clusters)
    far_rows = own[:, halo_far]
    near_in = passed_along(own, "gx", -1)
    far_in = passed_along(far_rows, "gx", -2)
    lift_rows = (jnp.arange(48) < 8)[:, None]
    near_in = near_in + jnp.where(lift_rows & (domain_index == axis_count - 1), box_lengths[0], 0.0)
    far_in = far_in + jnp.where(lift_rows & (domain_index >= axis_count - 2), box_lengths[0], 0.0)
    table = jnp.concatenate([own, near_in, far_in], axis=1)
    columns, virial_parts = pair_forces(pair_count, box_lengths, table, pair_list, exclusion, clusters)
    near_back = passed_along(columns[:, clusters : 2 * clusters], "gx", 1)
    far_back = passed_along(columns[:, 2 * clusters :], "gx", 2)
    kinetic = 0.5 * jnp.sum(velocities * velocities / inverse_mass[None, :], axis=1)
    virial = jnp.sum(virial_parts.reshape(3, 8 * LANES), axis=1)
    totals = lax.psum(jnp.concatenate([kinetic, virial]), "gx")
    kinetic, virial = totals[:3], totals[3:]
    summed = columns[:, :clusters] + near_back
    summed = summed.at[:, halo_far].add(far_back)
    forces = summed.reshape(3, 8, clusters).transpose(0, 2, 1).reshape(3, atoms_here)
    kinetic_sum = jnp.sum(kinetic)
    particles = atoms_here * axis_count
    volume = box_lengths[0] * box_lengths[1] * box_lengths[2]
    thermal_ratio = 2.0 * kinetic_sum / (3.0 * particles * thermal_scale_unit)
    damping = extended_variables[0] + reservoir_inertia_mass * (thermal_ratio - 1.0)
    box_rates = extended_variables[1:] + barostat_gain * (
        kinetic - virial - pressure_target * volume / 2.0
    ) / (kinetic_sum / 3.0)
    new_velocities = velocities + time_step * (
        forces * inverse_mass[None, :] - (damping + box_rates[:, None]) * velocities
    )
    new_positions = positions * (1.0 + time_step * box_rates[:, None]) + time_step * new_velocities
    new_coupling = jnp.concatenate([damping[None], box_rates])
    return (forces, new_velocities, new_positions, new_coupling)


def solution(mesh):
    return jax.shard_map(
        on_device,
        mesh=mesh,
        in_specs=(
            P(None, ("rep", "gx")),
            P(None, ("rep", "gx")),
            P(None, ("rep", "gx")),
            P(None, ("rep", "gx")),
            P(("rep", "gx")),
            P(None, ("rep", "gx")),
            P(("rep", "gx")),
            P("rep"),
            P("rep"),
        ),
        out_specs=(
            P(None, ("rep", "gx")),
            P(None, ("rep", "gx")),
            P(None, ("rep", "gx")),
            P("rep"),
        ),
        check_vma=False,
    )
```

```python
import functools

import jax
import jax.numpy as jnp
from jax import lax
from jax.experimental import pallas as pl
from jax.experimental.pallas import tpu as pltpu
from jax.sharding import PartitionSpec as P

time_step = 0.25
reaction_term = 1.0 / 1331.0
thermal_scale_unit = 2.0
reservoir_inertia_mass = 4.0
barostat_gain = 0.1
pressure_target = 1.0

F32 = jnp.float32
BF16 = jnp.bfloat16
LANES = 128


def passed_along(value, axis, steps):
    count = lax.axis_size(axis)
    pairs = [(source, (source + steps) % count) for source in range(count)]
    return lax.ppermute(value, axis, pairs)


def split_bf16(value, terms):
    parts = []
    for _ in range(terms - 1):
        part = value.astype(BF16)
        parts.append(part)
        value = value - part.astype(F32)
    parts.append(value.astype(BF16))
    return parts


def one_hot_rows(index_row, rows):
    width = index_row.shape[1]
    numbers = lax.broadcasted_iota(jnp.int16, (rows, width), 0)
    wanted = jnp.broadcast_to(index_row, (rows, width)).astype(jnp.int16)
    return jnp.where(numbers == wanted, jnp.ones((), BF16), jnp.zeros((), BF16))


def fold_rows(first, second, stride, lane_rows):
    keep = (lane_rows & stride) == 0
    return jnp.where(keep, first, second) + pltpu.roll(
        jnp.where(keep, second, first), 8 - stride, 0
    )


def pair_kernel(
    count_ref,
    scalar_ref,
    own_ref,
    near_ref,
    far_ref,
    velocity_ref,
    param_ref,
    pair_ref,
    word_ref,
    own_force_ref,
    near_force_ref,
    far_force_ref,
    energy_ref,
    parts_ref,
    onto_j,
    onto_i,
    *,
    width,
):
    slots = onto_j.shape[1]
    clusters = onto_i.shape[1]
    x_rows = (lax.broadcasted_iota(jnp.int32, (48, 1), 0) < 8).astype(F32)
    table = jnp.concatenate(
        [own_ref[...], near_ref[...] + x_rows * scalar_ref[0], far_ref[...] + x_rows * scalar_ref[1]],
        axis=1,
    )
    places = split_bf16(table[:24], 3)
    params = split_bf16(table[24:], 2)
    parts_ref[...] = jnp.concatenate([part.astype(F32) for part in places + params], axis=0).astype(BF16)
    onto_j[...] = jnp.zeros_like(onto_j)
    onto_i[...] = jnp.zeros_like(onto_i)
    total = count_ref[0]
    box_y = scalar_ref[2]
    box_z = scalar_ref[3]
    lane_rows = lax.broadcasted_iota(jnp.int32, (8, LANES), 0)

    def gathered(hot, rows):
        raw = jnp.dot(parts_ref[:, :rows], hot, preferred_element_type=F32)
        place = raw[0:24] + (raw[24:48] + raw[48:72])
        param = raw[72:96] + raw[96:120]
        return place, param

    def one_block(block, virial):
        start = pl.multiple_of(block * width, width)
        first = pair_ref[0:1, pl.ds(start, width)]
        second = pair_ref[1:2, pl.ds(start, width)]
        image = pair_ref[2:3, pl.ds(start, width)]
        words = word_ref[:, pl.ds(start, width)]
        column = start + lax.broadcasted_iota(jnp.int32, (1, width), 1)
        words = jnp.where(column < total, words, 0)
        image_row = (image >= 3).astype(jnp.int32) + (image >= 6).astype(jnp.int32)
        shift_y = (image_row - 1).astype(F32) * box_y
        shift_z = (image - 3 * image_row - 1).astype(F32) * box_z
        hot_i = one_hot_rows(first, clusters)
        hot_j = one_hot_rows(second, slots)
        place_i, param_i = gathered(hot_i, clusters)
        place_j, param_j = gathered(hot_j, slots)
        j_chunks = []
        i_chunks = []
        for chunk in range(width // LANES):
            cut = slice(chunk * LANES, (chunk + 1) * LANES)
            jx = place_j[0:8, cut]
            jy = place_j[8:16, cut] + shift_y[:, cut]
            jz = place_j[16:24, cut] + shift_z[:, cut]
            jq = param_j[0:8, cut]
            je = 6.0 * param_j[8:16, cut]
            jb = 12.0 * param_j[16:24, cut]
            force_j = [jnp.zeros((8, LANES), F32) for _ in range(3)]
            stack = []
            for a in range(8):
                if a % 2 == 0:
                    shifted = jnp.right_shift(
                        jnp.broadcast_to(words[a // 2 : a // 2 + 1, cut], (8, LANES)), lane_rows
                    )
                interact = (shifted & (1 if a % 2 == 0 else 256)) != 0
                delta = (
                    jx - place_i[a : a + 1, cut],
                    jy - place_i[8 + a : 9 + a, cut],
                    jz - place_i[16 + a : 17 + a, cut],
                )
                radius_sq = delta[0] * delta[0] + delta[1] * delta[1] + delta[2] * delta[2]
                inverse = lax.rsqrt(radius_sq)
                inverse_sq = inverse * inverse
                inverse_six = inverse_sq * inverse_sq * inverse_sq
                charge = jq * param_i[a : a + 1, cut]
                dispersion = je * param_i[8 + a : 9 + a, cut]
                repulsion = jb * param_i[16 + a : 17 + a, cut]
                scalar = charge * (inverse * inverse_sq - reaction_term) + (
                    repulsion * inverse_six - dispersion
                ) * (inverse_six * inverse_sq)
                scalar = jnp.where(interact, scalar, 0.0)
                force = [scalar * part for part in delta]
                force_j = [old + new for old, new in zip(force_j, force)]
                virial = tuple(old + f * d for old, f, d in zip(virial, force, delta))
                stack.append((1, force))
                while len(stack) > 1 and stack[-1][0] == stack[-2][0]:
                    stride, high = stack.pop()
                    _, low = stack.pop()
                    stack.append(
                        (2 * stride, [fold_rows(x, y, stride, lane_rows) for x, y in zip(low, high)])
                    )
            j_chunks.append(jnp.concatenate(force_j, axis=0))
            i_chunks.append(jnp.concatenate(stack[0][1], axis=0))
        sides = ((j_chunks, hot_j, onto_j), (i_chunks, hot_i, onto_i))
        for chunks, hot, target in sides:
            high, low = split_bf16(jnp.concatenate(chunks, axis=1), 2)
            pieces = jnp.concatenate([high.astype(F32), low.astype(F32)], axis=0).astype(BF16)
            target[...] += lax.dot_general(
                pieces, hot, (((1,), (1,)), ((), ())), preferred_element_type=F32
            )
        return virial

    blocks = (total + width - 1) // width
    zero = jnp.zeros((8, LANES), F32)
    virial = lax.fori_loop(0, blocks, one_block, (zero, zero, zero))
    onto = onto_j[0:24, :] + onto_j[24:48, :]
    own_force_ref[...] = onto[:, :clusters] - (onto_i[0:24, :] + onto_i[24:48, :])
    near_force_ref[...] = onto[:, clusters : 2 * clusters]
    far_force_ref[...] = onto[:, 2 * clusters :]
    speed = velocity_ref[...]
    motion = jnp.sum(0.5 * speed * speed / param_ref[3:4, :], axis=1, keepdims=True)
    lane = lax.broadcasted_iota(jnp.int32, (3, LANES), 1)
    energy_ref[0:3, :] = jnp.where(lane == 0, motion, 0.0)
    for c in range(3):
        energy_ref[3 + c : 4 + c, :] = -0.5 * jnp.sum(virial[c], axis=0, keepdims=True)
    energy_ref[6:8, :] = jnp.zeros((2, LANES), F32)


def pair_forces(pair_count, scalars, own, near, far, velocities, atom_params, pair_list, exclusion):
    columns = pair_list.shape[1]
    width = next(w for w in (512, 256, 128) if columns % w == 0)
    clusters = own.shape[1]
    far_clusters = far.shape[1]
    slots = 2 * clusters + far_clusters
    vmem = pl.BlockSpec(memory_space=pltpu.VMEM)
    smem = pl.BlockSpec(memory_space=pltpu.SMEM)
    return pl.pallas_call(
        functools.partial(pair_kernel, width=width),
        out_shape=(
            jax.ShapeDtypeStruct((24, clusters), F32),
            jax.ShapeDtypeStruct((24, clusters), F32),
            jax.ShapeDtypeStruct((24, far_clusters), F32),
            jax.ShapeDtypeStruct((8, LANES), F32),
        ),
        in_specs=[smem, smem] + [vmem] * 7,
        out_specs=(vmem,) * 4,
        scratch_shapes=[
            pltpu.VMEM((120, slots), BF16),
            pltpu.VMEM((48, slots), F32),
            pltpu.VMEM((48, clusters), F32),
        ],
        name="pair_forces",
    )(pair_count, scalars, own, near, far, velocities, atom_params, pair_list, exclusion)


def summed_over(value, axis):
    count = lax.axis_size(axis)
    if count & (count - 1):
        return jnp.sum(lax.all_gather(value, axis), axis=0)
    stride = 1
    while stride < count:
        pairs = [(source, source ^ stride) for source in range(count)]
        value = value + lax.ppermute(value, axis, pairs)
        stride *= 2
    return value


def on_device(
    positions,
    velocities,
    atom_params,
    pair_list,
    pair_count,
    exclusion,
    halo_far,
    box_lengths,
    extended_variables,
):
    atoms_here = positions.shape[1]
    clusters = atoms_here // 8
    domain_index = lax.axis_index("gx")
    axis_count = lax.axis_size("gx")
    inverse_mass = atom_params[3]
    packed = jnp.concatenate([positions, atom_params[:3]], axis=0)
    own = packed.reshape(6, clusters, 8).transpose(0, 2, 1).reshape(48, clusters)
    far_rows = own[:, halo_far]
    near_in = passed_along(own, "gx", -1)
    far_in = passed_along(far_rows, "gx", -2)
    scalars = jnp.stack(
        [
            jnp.where(domain_index == axis_count - 1, box_lengths[0], 0.0),
            jnp.where(domain_index >= axis_count - 2, box_lengths[0], 0.0),
            box_lengths[1],
            box_lengths[2],
        ]
    )
    own_force, near_force, far_force, energies = pair_forces(
        pair_count, scalars, own, near_in, far_in, velocities, atom_params, pair_list, exclusion
    )
    near_back = passed_along(near_force, "gx", 1)
    far_back = passed_along(far_force, "gx", 2)
    totals = jnp.sum(summed_over(energies, "gx"), axis=1)
    kinetic, virial = totals[:3], totals[3:6]
    summed = own_force + near_back
    summed = summed.at[:, halo_far].add(far_back)
    forces = summed.reshape(3, 8, clusters).transpose(0, 2, 1).reshape(3, atoms_here)
    kinetic_sum = jnp.sum(kinetic)
    particles = atoms_here * axis_count
    volume = box_lengths[0] * box_lengths[1] * box_lengths[2]
    thermal_ratio = 2.0 * kinetic_sum / (3.0 * particles * thermal_scale_unit)
    damping = extended_variables[0] + reservoir_inertia_mass * (thermal_ratio - 1.0)
    box_rates = extended_variables[1:] + barostat_gain * (
        kinetic - virial - pressure_target * volume / 2.0
    ) / (kinetic_sum / 3.0)
    new_velocities = velocities + time_step * (
        forces * inverse_mass[None, :] - (damping + box_rates[:, None]) * velocities
    )
    new_positions = positions * (1.0 + time_step * box_rates[:, None]) + time_step * new_velocities
    new_coupling = jnp.concatenate([damping[None], box_rates])
    return (forces, new_velocities, new_positions, new_coupling)


def solution(mesh):
    return jax.shard_map(
        on_device,
        mesh=mesh,
        in_specs=(
            P(None, ("rep", "gx")),
            P(None, ("rep", "gx")),
            P(None, ("rep", "gx")),
            P(None, ("rep", "gx")),
            P(("rep", "gx")),
            P(None, ("rep", "gx")),
            P(("rep", "gx")),
            P("rep"),
            P("rep"),
        ),
        out_specs=(
            P(None, ("rep", "gx")),
            P(None, ("rep", "gx")),
            P(None, ("rep", "gx")),
            P("rep"),
        ),
        check_vma=False,
    )
```

```python
import functools

import jax
import jax.numpy as jnp
from jax import lax
from jax.experimental import pallas as pl
from jax.experimental.pallas import tpu as pltpu
from jax.sharding import PartitionSpec as P

time_step = 0.25
reaction_term = 1.0 / 1331.0
thermal_scale_unit = 2.0
reservoir_inertia_mass = 4.0
barostat_gain = 0.1
pressure_target = 1.0

F32 = jnp.float32
BF16 = jnp.bfloat16
LANES = 128


def passed_along(value, axis, steps):
    count = lax.axis_size(axis)
    pairs = [(source, (source + steps) % count) for source in range(count)]
    return lax.ppermute(value, axis, pairs)


def split_bf16(value, terms):
    parts = []
    for _ in range(terms - 1):
        part = value.astype(BF16)
        parts.append(part)
        value = value - part.astype(F32)
    parts.append(value.astype(BF16))
    return parts


def one_hot_rows(index_row, rows):
    width = index_row.shape[1]
    numbers = lax.broadcasted_iota(jnp.int16, (rows, width), 0)
    wanted = jnp.broadcast_to(index_row, (rows, width)).astype(jnp.int16)
    return jnp.where(numbers == wanted, jnp.ones((), BF16), jnp.zeros((), BF16))


def fold_rows(first, second, stride, lane_rows):
    keep = (lane_rows & stride) == 0
    return jnp.where(keep, first, second) + pltpu.roll(
        jnp.where(keep, second, first), 8 - stride, 0
    )


def pair_kernel(
    count_ref,
    scalar_ref,
    own_ref,
    near_ref,
    far_ref,
    velocity_ref,
    param_ref,
    pair_ref,
    word_ref,
    own_force_ref,
    near_force_ref,
    far_force_ref,
    energy_ref,
    parts_ref,
    onto_j,
    onto_i,
    *,
    width,
):
    slots = onto_j.shape[1]
    clusters = onto_i.shape[1]
    x_rows = (lax.broadcasted_iota(jnp.int32, (48, 1), 0) < 8).astype(F32)
    table = jnp.concatenate(
        [own_ref[...], near_ref[...] + x_rows * scalar_ref[0], far_ref[...] + x_rows * scalar_ref[1]],
        axis=1,
    )
    places = split_bf16(table[:24], 3)
    params = split_bf16(table[24:], 2)
    parts_ref[...] = jnp.concatenate([part.astype(F32) for part in places + params], axis=0).astype(BF16)
    onto_j[...] = jnp.zeros_like(onto_j)
    onto_i[...] = jnp.zeros_like(onto_i)
    total = count_ref[0]
    box_y = scalar_ref[2]
    box_z = scalar_ref[3]
    lane_rows = lax.broadcasted_iota(jnp.int32, (8, LANES), 0)

    def gathered(hot, rows):
        raw = jnp.dot(parts_ref[:, :rows], hot, preferred_element_type=F32)
        place = raw[0:24] + (raw[24:48] + raw[48:72])
        param = raw[72:96] + raw[96:120]
        return place, param

    def one_block(block, virial):
        start = pl.multiple_of(block * width, width)
        first = pair_ref[0:1, pl.ds(start, width)]
        second = pair_ref[1:2, pl.ds(start, width)]
        image = pair_ref[2:3, pl.ds(start, width)]
        words = word_ref[:, pl.ds(start, width)]
        column = start + lax.broadcasted_iota(jnp.int32, (1, width), 1)
        words = jnp.where(column < total, words, 0)
        image_row = (image >= 3).astype(jnp.int32) + (image >= 6).astype(jnp.int32)
        shift_y = (image_row - 1).astype(F32) * box_y
        shift_z = (image - 3 * image_row - 1).astype(F32) * box_z
        hot_i = one_hot_rows(first, clusters)
        hot_j = one_hot_rows(second, slots)
        place_i, param_i = gathered(hot_i, clusters)
        place_j, param_j = gathered(hot_j, slots)
        j_chunks = []
        i_chunks = []
        for chunk in range(width // LANES):
            cut = slice(chunk * LANES, (chunk + 1) * LANES)
            jx = place_j[0:8, cut]
            jy = place_j[8:16, cut] + shift_y[:, cut]
            jz = place_j[16:24, cut] + shift_z[:, cut]
            jq = param_j[0:8, cut]
            je = 6.0 * param_j[8:16, cut]
            jb = 12.0 * param_j[16:24, cut]
            force_j = [jnp.zeros((8, LANES), F32) for _ in range(3)]
            stack = []
            for a in range(8):
                if a % 2 == 0:
                    shifted = jnp.right_shift(
                        jnp.broadcast_to(words[a // 2 : a // 2 + 1, cut], (8, LANES)), lane_rows
                    )
                interact = (shifted & (1 if a % 2 == 0 else 256)) != 0
                delta = (
                    jx - place_i[a : a + 1, cut],
                    jy - place_i[8 + a : 9 + a, cut],
                    jz - place_i[16 + a : 17 + a, cut],
                )
                radius_sq = delta[0] * delta[0] + delta[1] * delta[1] + delta[2] * delta[2]
                inverse = lax.rsqrt(radius_sq)
                inverse_sq = inverse * inverse
                inverse_six = inverse_sq * inverse_sq * inverse_sq
                charge = jq * param_i[a : a + 1, cut]
                dispersion = je * param_i[8 + a : 9 + a, cut]
                repulsion = jb * param_i[16 + a : 17 + a, cut]
                scalar = charge * (inverse * inverse_sq - reaction_term) + (
                    repulsion * inverse_six - dispersion
                ) * (inverse_six * inverse_sq)
                scalar = jnp.where(interact, scalar, 0.0)
                force = [scalar * part for part in delta]
                force_j = [old + new for old, new in zip(force_j, force)]
                virial = tuple(old + f * d for old, f, d in zip(virial, force, delta))
                stack.append((1, force))
                while len(stack) > 1 and stack[-1][0] == stack[-2][0]:
                    stride, high = stack.pop()
                    _, low = stack.pop()
                    stack.append(
                        (2 * stride, [fold_rows(x, y, stride, lane_rows) for x, y in zip(low, high)])
                    )
            j_chunks.append(jnp.concatenate(force_j, axis=0))
            i_chunks.append(jnp.concatenate(stack[0][1], axis=0))
        sides = ((j_chunks, hot_j, onto_j), (i_chunks, hot_i, onto_i))
        for chunks, hot, target in sides:
            high, low = split_bf16(jnp.concatenate(chunks, axis=1), 2)
            pieces = jnp.concatenate([high.astype(F32), low.astype(F32)], axis=0).astype(BF16)
            target[...] += lax.dot_general(
                pieces, hot, (((1,), (1,)), ((), ())), preferred_element_type=F32
            )
        return virial

    blocks = (total + width - 1) // width
    zero = jnp.zeros((8, LANES), F32)
    virial = lax.fori_loop(0, blocks, one_block, (zero, zero, zero))
    onto = onto_j[0:24, :] + onto_j[24:48, :]
    own_force_ref[...] = onto[:, :clusters] - (onto_i[0:24, :] + onto_i[24:48, :])
    near_force_ref[...] = onto[:, clusters : 2 * clusters]
    far_force_ref[...] = onto[:, 2 * clusters :]
    speed = velocity_ref[...]
    motion = jnp.sum(0.5 * speed * speed / param_ref[3:4, :], axis=1, keepdims=True)
    lane = lax.broadcasted_iota(jnp.int32, (3, LANES), 1)
    energy_ref[0:3, :] = jnp.where(lane == 0, motion, 0.0)
    for c in range(3):
        energy_ref[3 + c : 4 + c, :] = -0.5 * jnp.sum(virial[c], axis=0, keepdims=True)
    energy_ref[6:8, :] = jnp.zeros((2, LANES), F32)


def pair_forces(pair_count, scalars, own, near, far, velocities, atom_params, pair_list, exclusion):
    columns = pair_list.shape[1]
    width = next(w for w in (512, 256, 128) if columns % w == 0)
    clusters = own.shape[1]
    far_clusters = far.shape[1]
    slots = 2 * clusters + far_clusters
    vmem = pl.BlockSpec(memory_space=pltpu.VMEM)
    smem = pl.BlockSpec(memory_space=pltpu.SMEM)
    return pl.pallas_call(
        functools.partial(pair_kernel, width=width),
        out_shape=(
            jax.ShapeDtypeStruct((24, clusters), F32),
            jax.ShapeDtypeStruct((24, clusters), F32),
            jax.ShapeDtypeStruct((24, far_clusters), F32),
            jax.ShapeDtypeStruct((8, LANES), F32),
        ),
        in_specs=[smem, smem] + [vmem] * 7,
        out_specs=(vmem,) * 4,
        scratch_shapes=[
            pltpu.VMEM((120, slots), BF16),
            pltpu.VMEM((48, slots), F32),
            pltpu.VMEM((48, clusters), F32),
        ],
        name="pair_forces",
    )(pair_count, scalars, own, near, far, velocities, atom_params, pair_list, exclusion)


def summed_over(value, axis):
    count = lax.axis_size(axis)
    if count & (count - 1):
        return jnp.sum(lax.all_gather(value, axis), axis=0)
    stride = 1
    while stride < count:
        pairs = [(source, source ^ stride) for source in range(count)]
        value = value + lax.ppermute(value, axis, pairs)
        stride *= 2
    return value


def update_kernel(
    box_ref,
    extended_ref,
    own_ref,
    near_ref,
    far_ref,
    halo_ref,
    energy_ref,
    position_ref,
    velocity_ref,
    param_ref,
    force_ref,
    new_velocity_ref,
    new_position_ref,
    coupling_ref,
    spread_ref,
    *,
    particles,
):
    clusters = own_ref.shape[1]
    far_clusters = far_ref.shape[1]
    numbers = lax.broadcasted_iota(jnp.int32, (clusters, far_clusters), 0)
    hot = (numbers == halo_ref[...]).astype(F32)
    summed = own_ref[...] + near_ref[...]
    summed = summed + lax.dot_general(
        far_ref[...],
        hot,
        (((1,), (1,)), ((), ())),
        precision=lax.Precision.HIGHEST,
        preferred_element_type=F32,
    )
    padded = jnp.concatenate([summed, jnp.zeros((LANES - 24, clusters), F32)], axis=0)
    turned = padded.T
    for k in range(8):
        moved = turned if k == 0 else pltpu.roll(turned, LANES - k, 1)
        spread_ref[pl.ds(k, clusters, stride=8), :] = moved
    force_rows = spread_ref[...].T
    totals = jnp.sum(energy_ref[...], axis=1, keepdims=True)
    kinetic = [totals[c : c + 1] for c in range(3)]
    kinetic_sum = kinetic[0] + kinetic[1] + kinetic[2]
    volume = box_ref[0] * box_ref[1] * box_ref[2]
    thermal_ratio = 2.0 * kinetic_sum / (3.0 * particles * thermal_scale_unit)
    damping = extended_ref[0] + reservoir_inertia_mass * (thermal_ratio - 1.0)
    inverse_mass = param_ref[3:4, :]
    coupling = [damping]
    for c in range(3):
        rate = extended_ref[1 + c] + barostat_gain * (
            kinetic[c] - totals[3 + c : 4 + c] - pressure_target * volume / 2.0
        ) / (kinetic_sum / 3.0)
        force = force_rows[8 * c : 8 * c + 1]
        velocity = velocity_ref[c : c + 1, :]
        new_velocity = velocity + time_step * (force * inverse_mass - (damping + rate) * velocity)
        force_ref[c : c + 1, :] = force
        new_velocity_ref[c : c + 1, :] = new_velocity
        new_position_ref[c : c + 1, :] = (
            position_ref[c : c + 1, :] * (1.0 + time_step * rate) + time_step * new_velocity
        )
        coupling.append(rate)
    coupling_ref[...] = jnp.concatenate(coupling, axis=1)


def updated(
    own_force,
    near_back,
    far_back,
    halo_far,
    energies,
    positions,
    velocities,
    atom_params,
    box_lengths,
    extended_variables,
    particles,
):
    atoms_here = positions.shape[1]
    vmem = pl.BlockSpec(memory_space=pltpu.VMEM)
    smem = pl.BlockSpec(memory_space=pltpu.SMEM)
    rows = jax.ShapeDtypeStruct((3, atoms_here), F32)
    forces, new_velocities, new_positions, coupling = pl.pallas_call(
        functools.partial(update_kernel, particles=particles),
        out_shape=(rows, rows, rows, jax.ShapeDtypeStruct((1, 4), F32)),
        in_specs=[smem, smem] + [vmem] * 8,
        out_specs=(vmem,) * 4,
        scratch_shapes=[pltpu.VMEM((atoms_here, LANES), F32)],
        name="update",
    )(
        box_lengths,
        extended_variables,
        own_force,
        near_back,
        far_back,
        halo_far[None, :],
        energies,
        positions,
        velocities,
        atom_params,
    )
    return (forces, new_velocities, new_positions, coupling[0])


def on_device(
    positions,
    velocities,
    atom_params,
    pair_list,
    pair_count,
    exclusion,
    halo_far,
    box_lengths,
    extended_variables,
):
    atoms_here = positions.shape[1]
    clusters = atoms_here // 8
    domain_index = lax.axis_index("gx")
    axis_count = lax.axis_size("gx")
    packed = jnp.concatenate([positions, atom_params[:3]], axis=0)
    own = packed.reshape(6, clusters, 8).transpose(0, 2, 1).reshape(48, clusters)
    far_rows = own[:, halo_far]
    near_in = passed_along(own, "gx", -1)
    far_in = passed_along(far_rows, "gx", -2)
    scalars = jnp.stack(
        [
            jnp.where(domain_index == axis_count - 1, box_lengths[0], 0.0),
            jnp.where(domain_index >= axis_count - 2, box_lengths[0], 0.0),
            box_lengths[1],
            box_lengths[2],
        ]
    )
    own_force, near_force, far_force, energies = pair_forces(
        pair_count, scalars, own, near_in, far_in, velocities, atom_params, pair_list, exclusion
    )
    near_back = passed_along(near_force, "gx", 1)
    far_back = passed_along(far_force, "gx", 2)
    energies = summed_over(energies, "gx")
    return updated(
        own_force,
        near_back,
        far_back,
        halo_far,
        energies,
        positions,
        velocities,
        atom_params,
        box_lengths,
        extended_variables,
        atoms_here * axis_count,
    )


def solution(mesh):
    return jax.shard_map(
        on_device,
        mesh=mesh,
        in_specs=(
            P(None, ("rep", "gx")),
            P(None, ("rep", "gx")),
            P(None, ("rep", "gx")),
            P(None, ("rep", "gx")),
            P(("rep", "gx")),
            P(None, ("rep", "gx")),
            P(("rep", "gx")),
            P("rep"),
            P("rep"),
        ),
        out_specs=(
            P(None, ("rep", "gx")),
            P(None, ("rep", "gx")),
            P(None, ("rep", "gx")),
            P("rep"),
        ),
        check_vma=False,
    )
```
